32 devices in a mesh: lat: 4 (over y, core), lon: 4 (over z), lev: 2 (over x).
Axes of the slice: x: 2, y: 2, z: 4, core: 2. Of those that a mesh axis runs over, the one named last changes fastest.
Arguments:
- density: float32 [128, 16, 256, 128], P('lat', 'lon', 'lev'), may hold values from 0.2 to 1.8
- crowding: float32 [128, 16, 256, 128], P('lat', 'lon', 'lev'), may hold values from 0.5 to 2
Outputs:
- running_total: float32 [128, 16, 256, 128], P('lat', 'lon', 'lev')
- density_end: float32 [128, 16, 256, 128], P('lat', 'lon', 'lev')
The draws below stay inside these ranges and needn't reach their ends.
All inputs are finite; a program needn't handle non-finite values.
Results may differ from the reference program's by a relative error of at most 0.00002.
Values sent between devices are 32-bit elements; how exact they have to be, the bound alone decides.
A program may use at most 320 MiB of HBM per device.

```python
import jax
import jax.numpy as jnp
from jax import lax

GRID_J = 128
GRID_I = 16
GRID_K = 256
LEVELS = 128
STEPS = 4


def level_of(stream_key, shape, split, smallest, largest):
    level, own = 1.0, jax.random.fold_in(stream_key, 6)
    for dim, shards_of in split:
        heights = jnp.exp(jax.random.uniform(jax.random.fold_in(own, dim), (shards_of,), jnp.float32, smallest / len(split), largest / len(split)))
        level = level * jnp.repeat(heights, shape[dim] // shards_of).reshape([-1 if axis == dim else 1 for axis in range(len(shape))])
    return level


def setup_inputs(seed: int = 0) -> dict:
    key_list = jax.random.split(jax.random.key(seed), 3)
    density = jnp.clip(0.2 + 1.5999999 * jax.random.uniform(key_list[0], (GRID_J, GRID_I, GRID_K, LEVELS), jnp.float32) ** level_of(key_list[0], (GRID_J, GRID_I, GRID_K, LEVELS), ((0, 4), (1, 4), (2, 2)), -0.2, 0.2), 0.2, 1.8)
    crowding = jnp.clip(0.5 + 1.5 * jax.random.uniform(key_list[1], (GRID_J, GRID_I, GRID_K, LEVELS), jnp.float32) ** level_of(key_list[1], (GRID_J, GRID_I, GRID_K, LEVELS), ((0, 4), (1, 4), (2, 2)), -0.2, 0.2), 0.5, 2.0)
    return dict(density=density, crowding=crowding)


def without_rim(values, dims):
    for dim in dims:
        values = lax.slice_in_dim(values, 1, values.shape[dim] - 1, axis=dim)
    return values


def shifted_cells(values, dim, start, dims):
    others = [other for other in dims if other != dim]
    values = without_rim(values, others)
    return lax.slice_in_dim(values, start, start + values.shape[dim] - 2, axis=dim)


def march_step(padded, crowding):
    middle = without_rim(padded, (0, 1, 2))
    lower = [shifted_cells(padded, dim, 0, (0, 1, 2)) for dim in (0, 1, 2)]
    upper = [shifted_cells(padded, dim, 2, (0, 1, 2)) for dim in (0, 1, 2)]
    spread = lower[0] + upper[0] + lower[1] + upper[1] + lower[2] + upper[2] - 6.0 * middle
    return middle + 0.1 * spread + 0.2 * middle * (1.0 - middle * crowding)


def reference(density, crowding):
    for step in range(STEPS):
        density = march_step(jnp.pad(density, ((1, 1), (1, 1), (1, 1), (0, 0)), mode="wrap"), crowding)
    running_total = jnp.cumsum(density, axis=1) / GRID_I
    return running_total, density
```

```python
import functools

import jax
import jax.numpy as jnp
from jax import lax
from jax.experimental import pallas as pl
from jax.experimental.pallas import tpu as pltpu
from jax.sharding import PartitionSpec as P

STEPS = 4
CHUNKS = 16
LEAD = 6
EXTRA = 4
PART = 1
MESH = pl.DeviceIdType.MESH
LO, HI = 0, 1


def loop(count, act):
    def lap(c, carry):
        act(c)
        return carry

    lax.fori_loop(0, count, lap, 0)


def kernel(
    sizes, density, crowding, running, density_end,
    field, crowd, lon, below, lev,
    load_sem, crowd_sem,
    lon_send, lon_recv, lev_send, lev_recv, lat_send, lat_recv, total_send, total_recv, credit,
):
    n_lat, n_lon, n_lev = sizes
    J, I, K, L = density.shape
    rows = max(1, J // CHUNKS)
    chunks = J // rows
    names = {"lat": n_lat, "lon": n_lon, "lev": n_lev}
    me = {name: lax.axis_index(name) for name in names}
    near = {
        name: (
            {name: lax.rem(me[name] + n - 1, n)},
            {name: lax.rem(me[name] + 1, n)},
        )
        for name, n in names.items()
    }

    def load(c):
        own = pl.ds(c * rows, rows)
        return pltpu.make_async_copy(density.at[own], field.at[0, pl.ds(1 + c * rows, rows)], load_sem.at[c])

    def load_crowd():
        return pltpu.make_async_copy(crowding, crowd, crowd_sem)

    def remote(src, dst, send_sem, recv_sem, name, side):
        return pltpu.make_async_remote_copy(
            src_ref=src,
            dst_ref=dst,
            send_sem=send_sem,
            recv_sem=recv_sem,
            device_id=near[name][side],
            device_id_type=MESH,
        )

    def lon_copy(slot, side, c):
        own = pl.ds(c * rows, rows)
        plane = 0 if side == LO else I - 1
        return remote(
            field.at[slot, pl.ds(1 + c * rows, rows), plane], lon.at[1 - side, own],
            lon_send.at[slot], lon_recv.at[c], "lon", side,
        )

    def lon_both(slot, c):
        own = lon.at[:, pl.ds(c * rows, rows)]
        return remote(own, own, lon_send.at[slot], lon_recv.at[c], "lon", HI)

    def lon_all(slot):
        return remote(lon, lon, lon_send.at[slot], lon_recv.at[0], "lon", HI)

    def total_copy(p):
        own = pl.ds(p * PART, PART)
        return remote(
            running.at[own, I - 1], below.at[own], total_send, total_recv.at[p], "lon", HI
        )

    def total_all():
        return remote(below, below, total_send, total_recv.at[0], "lon", HI)

    def lev_copy(slot, side, c):
        own = pl.ds(c * rows, rows)
        first = 0 if side == LO else K - 8
        return remote(
            field.at[slot, pl.ds(1 + c * rows, rows), :, pl.ds(first, 8)], lev.at[slot, 1 - side, own],
            lev_send.at[slot], lev_recv.at[slot, c], "lev", side,
        )

    def lev_both(slot, c):
        own = lev.at[slot, :, pl.ds(c * rows, rows)]
        return remote(own, own, lev_send.at[slot], lev_recv.at[slot, c], "lev", HI)

    def lev_all(slot):
        return remote(lev.at[slot], lev.at[slot], lev_send.at[slot], lev_recv.at[slot, 0], "lev", HI)

    def lat_copy(slot, side):
        return remote(
            field.at[slot, 1 if side == LO else J], field.at[slot, J + 1 if side == LO else 0],
            lat_send.at[side], lat_recv.at[slot, 1 - side], "lat", side,
        )

    def at_edges(c, act):
        @pl.when(c == 0)
        def _():
            act(LO)

        @pl.when(c == chunks - 1)
        def _():
            act(HI)

    def start_sides(slot, c):
        for side in (LO, HI):
            lev_copy(slot, side, c).start()
        at_edges(c, lambda side: lat_copy(slot, side).start())

    def end_receives(slot, c):
        lon_both(slot, c).wait_recv()
        lev_both(slot, c).wait_recv()
        at_edges(c, lambda side: lat_copy(slot, 1 - side).wait_recv())

    def trade_credit(c):
        for side in (LO, HI):
            pl.semaphore_signal(credit.at[c], inc=1, device_id=near["lon"][side], device_id_type=MESH)
        pl.semaphore_wait(credit.at[c], 2)

    barrier = pltpu.get_barrier_semaphore()
    for name in names:
        for side in (LO, HI):
            pl.semaphore_signal(barrier, inc=1, device_id=near[name][side], device_id_type=MESH)
    loop(chunks, lambda c: load(c).start())
    pl.semaphore_wait(barrier, 2 * len(names))

    def first(c):
        load(c).wait()
        for side in (LO, HI):
            lon_copy(0, side, c).start()
        start_sides(0, c)

    loop(chunks, first)
    load_crowd().start()

    at_k = lax.broadcasted_iota(jnp.int32, (K, L), 0)

    def advance(slot, j, put):
        for i in range(I):
            middle = field[slot, j + 1, i]
            lower = lon[LO, j] if i == 0 else field[slot, j + 1, i - 1]
            upper = lon[HI, j] if i == I - 1 else field[slot, j + 1, i + 1]
            before = jnp.where(at_k == 0, lev[slot, LO, j, i, 7:8], pltpu.roll(middle, 1, 0))
            after = jnp.where(at_k == K - 1, lev[slot, HI, j, i, 0:1], pltpu.roll(middle, K - 1, 0))
            around = (field[slot, j, i] + field[slot, j + 2, i]) + (lower + upper) + (before + after)
            put(j, i, middle * (0.6 - 0.2 * (middle * crowd[j, i])) + 0.1 * around)

    share = 1.0 / (I * n_lon)
    start = me["lon"] == 0
    end = me["lon"] == n_lon - 1
    lead = jnp.where(end, chunks, jnp.minimum(LEAD + EXTRA * me["lon"], chunks))

    def total(j):
        so_far = jnp.where(me["lon"] > 0, below[j], 0.0)
        for i in range(I):
            so_far = so_far + density_end[j, i] * share
            running[j, i] = so_far

    def put_field(slot):
        def put(j, i, value):
            field[slot, j + 1, i] = value

        return put

    def put_end(j, i, value):
        density_end[j, i] = value

    def march(step, c):
        slot = step % 2
        end_receives(slot, c)
        loop(rows, lambda r: advance(slot, c * rows + r, put_field(1 - slot)))
        at_edges(c, lambda side: lat_copy(slot, side).wait_send())
        start_sides(1 - slot, c)
        trade_credit(c)
        if step < STEPS - 2:
            for side in (LO, HI):
                lon_copy(1 - slot, side, c).start()
            return

        @pl.when(jnp.logical_not(start))
        def _():
            lon_copy(1 - slot, LO, c).start()

        @pl.when(c >= chunks - lead)
        def _():
            lon_copy(1 - slot, HI, c - (chunks - lead)).start()

    def march_last(c):
        slot = (STEPS - 1) % 2
        end_receives(slot, c)
        loop(rows, lambda r: advance(slot, c * rows + r, put_end))

        @pl.when(c < chunks - lead)
        def _():
            lon_copy(slot, HI, c + lead).start()

        def add_up(r):
            p = c * (rows // PART) + r

            @pl.when(jnp.logical_not(start))
            def _():
                total_copy(p).wait_recv()

            for q in range(PART):
                total(p * PART + q)

            @pl.when(jnp.logical_not(end))
            def _():
                total_copy(p).start()

        loop(rows // PART, add_up)

        @pl.when(start)
        def _():
            lon_copy(slot, LO, c).start()

    load_crowd().wait()
    for step in range(STEPS - 1):
        loop(chunks, lambda c: march(step, c))
        lon_all(step % 2).wait_send()
        lev_all(step % 2).wait_send()
    loop(chunks, march_last)
    slot = (STEPS - 1) % 2
    lon_all(slot).wait_send()
    lev_all(slot).wait_send()
    for side in (LO, HI):
        lat_copy(slot, side).wait_send()

    @pl.when(jnp.logical_not(end))
    def _():
        total_all().wait_send()


def body(sizes, density, crowding):
    J, I, K, L = density.shape
    chunks = J // max(1, J // CHUNKS)
    shape = pltpu.VMEM(density.shape, jnp.float32)
    dma = pltpu.SemaphoreType.DMA
    return pl.pallas_call(
        functools.partial(kernel, sizes),
        out_shape=(shape, shape),
        in_specs=[pl.BlockSpec(memory_space=pl.ANY)] * 2,
        out_specs=(pl.BlockSpec(memory_space=pltpu.VMEM),) * 2,
        scratch_shapes=[
            pltpu.VMEM((2, J + 2, I, K, L), jnp.float32),
            pltpu.VMEM((J, I, K, L), jnp.float32),
            pltpu.VMEM((2, J, K, L), jnp.float32),
            pltpu.VMEM((J, K, L), jnp.float32),
            pltpu.VMEM((2, 2, J, I, 8, L), jnp.float32),
            dma((chunks,)),
            dma,
            dma((2,)),
            dma((chunks,)),
            dma((2,)),
            dma((2, chunks)),
            dma((2,)),
            dma((2, 2)),
            dma,
            dma((J // PART,)),
            pltpu.SemaphoreType.REGULAR((chunks,)),
        ],
        compiler_params=pltpu.CompilerParams(
            collective_id=0, has_side_effects=True, vmem_limit_bytes=42 * 2**20
        ),
    )(density, crowding)


def solution(mesh):
    sizes = tuple(mesh.shape[name] for name in ("lat", "lon", "lev"))
    return jax.shard_map(
        functools.partial(body, sizes),
        mesh=mesh,
        in_specs=(P("lat", "lon", "lev", None), P("lat", "lon", "lev", None)),
        out_specs=(P("lat", "lon", "lev", None), P("lat", "lon", "lev", None)),
        check_vma=False,
    )
```

```python
import functools

import jax
import jax.numpy as jnp
from jax import lax
from jax.experimental import pallas as pl
from jax.experimental.pallas import tpu as pltpu
from jax.sharding import PartitionSpec as P

STEPS = 4
BULK = 16
FINE = 32
LEAD = 12
EXTRA = 8
PIECES = 4
LOADS = 8
EDGES = 4
STORES = 8
MESH = pl.DeviceIdType.MESH
LO, HI = 0, 1


def cut(length, count):
    size = max(1, length // count)
    return size, length // size


def loop(count, act):
    def lap(c, carry):
        act(c)
        return carry

    lax.fori_loop(0, count, lap, 0)


def kernel(
    sizes, density, crowding, carry, density_end,
    field, crowd, lon, below, totals, lev,
    load_sem, crowd_sem, lon_send, lon_recv, lev_send, lev_recv,
    lat_send, lat_recv, total_send, total_recv, piece_recv, credit,
):
    n_lat, n_lon, n_lev = sizes
    J, I, K, L = density.shape
    rows, chunks = cut(J, BULK)
    some, parts = cut(rows, max(1, FINE // chunks))
    fine = chunks * parts
    batch, batches = cut(chunks, LOADS)
    span, spans = cut(chunks, EDGES)
    names = {"lat": n_lat, "lon": n_lon, "lev": n_lev}
    me = {name: lax.axis_index(name) for name in names}
    near = {
        name: (
            {name: lax.rem(me[name] + n - 1, n)},
            {name: lax.rem(me[name] + 1, n)},
        )
        for name, n in names.items()
    }

    def load(c):
        first, count = c * batch * rows, batch * rows
        return pltpu.make_async_copy(
            density.at[pl.ds(first, count)], field.at[0, pl.ds(1 + first, count)], load_sem.at[c]
        )

    def load_crowd():
        return pltpu.make_async_copy(crowding, crowd, crowd_sem)

    def remote(src, dst, send_sem, recv_sem, name, side):
        return pltpu.make_async_remote_copy(
            src_ref=src,
            dst_ref=dst,
            send_sem=send_sem,
            recv_sem=recv_sem,
            device_id=near[name][side],
            device_id_type=MESH,
        )

    def lon_copy(slot, side, first, count, recv_sem):
        plane = 0 if side == LO else I - 1
        return remote(
            field.at[slot, pl.ds(1 + first, count), plane], lon.at[1 - side, pl.ds(first, count)],
            lon_send.at[slot], recv_sem, "lon", side,
        )

    def lon_bulk(slot, side, c):
        return lon_copy(slot, side, c * rows, rows, lon_recv.at[c * parts])

    def lon_fine(side, f):
        return lon_copy((STEPS - 1) % 2, side, f * some, some, lon_recv.at[f])

    def lon_both(first, count, recv_sem):
        own = lon.at[:, pl.ds(first, count)]
        return remote(own, own, lon_send.at[0], recv_sem, "lon", HI)

    def lon_all(slot):
        return remote(lon, lon, lon_send.at[slot], lon_recv.at[0], "lon", HI)

    def total_copy(f):
        own = pl.ds(f * some, some)
        return remote(totals.at[own], below.at[own], total_send, total_recv.at[f], "lon", HI)

    def piece_copy(j, p):
        own = pl.ds(p * (K // PIECES), K // PIECES)
        return remote(
            totals.at[j, own], below.at[j, own], total_send, piece_recv.at[j - (J - some), p], "lon", HI
        )

    def total_all():
        return remote(below, below, total_send, total_recv.at[0], "lon", HI)

    def lev_copy(slot, side, g):
        start, count = g * span * rows, span * rows
        first = 0 if side == LO else K - 8
        return remote(
            field.at[slot, pl.ds(1 + start, count), :, pl.ds(first, 8)],
            lev.at[slot, 1 - side, pl.ds(start, count)],
            lev_send.at[slot], lev_recv.at[slot, g], "lev", side,
        )

    def lev_both(slot, g):
        own = lev.at[slot, :, pl.ds(g * span * rows, span * rows)]
        return remote(own, own, lev_send.at[slot], lev_recv.at[slot, g], "lev", HI)

    def lev_all(slot):
        return remote(lev.at[slot], lev.at[slot], lev_send.at[slot], lev_recv.at[slot, 0], "lev", HI)

    def lat_copy(slot, side):
        return remote(
            field.at[slot, 1 if side == LO else J], field.at[slot, J + 1 if side == LO else 0],
            lat_send.at[side], lat_recv.at[slot, 1 - side], "lat", side,
        )

    def at_edges(c, act):
        @pl.when(c == 0)
        def _():
            act(LO)

        @pl.when(c == chunks - 1)
        def _():
            act(HI)

    def start_sides(slot, c):
        @pl.when(lax.rem(c, span) == span - 1)
        def _():
            for side in (LO, HI):
                lev_copy(slot, side, lax.div(c, span)).start()

        at_edges(c, lambda side: lat_copy(slot, side).start())

    def end_receives(slot, c):
        @pl.when(lax.rem(c, span) == 0)
        def _():
            lev_both(slot, lax.div(c, span)).wait_recv()

        at_edges(c, lambda side: lat_copy(slot, 1 - side).wait_recv())

    def trade_credit(c):
        for side in (LO, HI):
            pl.semaphore_signal(credit.at[c], inc=1, device_id=near["lon"][side], device_id_type=MESH)
        pl.semaphore_wait(credit.at[c], 2)

    barrier = pltpu.get_barrier_semaphore()
    for name in names:
        for side in (LO, HI):
            pl.semaphore_signal(barrier, inc=1, device_id=near[name][side], device_id_type=MESH)
    loop(batches, lambda c: load(c).start())
    pl.semaphore_wait(barrier, 2 * len(names))

    def first(c):
        @pl.when(lax.rem(c, batch) == 0)
        def _():
            load(lax.div(c, batch)).wait()

        for side in (LO, HI):
            lon_bulk(0, side, c).start()
        start_sides(0, c)

    loop(chunks, first)
    load_crowd().start()

    at_k = lax.broadcasted_iota(jnp.int32, (K, L), 0)

    def advance(slot, j, put):
        for i in range(I):
            middle = field[slot, j + 1, i]
            lower = lon[LO, j] if i == 0 else field[slot, j + 1, i - 1]
            upper = lon[HI, j] if i == I - 1 else field[slot, j + 1, i + 1]
            before = jnp.where(at_k == 0, lev[slot, LO, j, i, 7:8], pltpu.roll(middle, 1, 0))
            after = jnp.where(at_k == K - 1, lev[slot, HI, j, i, 0:1], pltpu.roll(middle, K - 1, 0))
            around = (field[slot, j, i] + field[slot, j + 2, i]) + (lower + upper) + (before + after)
            put(j, i, middle * (0.6 - 0.2 * (middle * crowd[j, i])) + 0.1 * around)

    share = 1.0 / (I * n_lon)
    start = me["lon"] == 0
    end = me["lon"] == n_lon - 1
    lead = jnp.where(end, fine, jnp.minimum(LEAD + EXTRA * me["lon"], fine))

    def add_up(j, own):
        so_far = jnp.where(me["lon"] > 0, below[j, own], 0.0)
        carry[j, own] = so_far
        for i in range(I):
            so_far = so_far + density_end[j, i, own] * share
        totals[j, own] = so_far

    def pass_on(copy, act):
        @pl.when(jnp.logical_not(start))
        def _():
            copy.wait_recv()

        act()

        @pl.when(jnp.logical_not(end))
        def _():
            copy.start()

    def put_field(slot):
        def put(j, i, value):
            field[slot, j + 1, i] = value

        return put

    def put_end(j, i, value):
        density_end[j, i] = value

    def march(step, c):
        slot = step % 2
        lon_both(c * rows, rows, lon_recv.at[c * parts]).wait_recv()
        end_receives(slot, c)
        loop(rows, lambda r: advance(slot, c * rows + r, put_field(1 - slot)))
        at_edges(c, lambda side: lat_copy(slot, side).wait_send())
        start_sides(1 - slot, c)
        trade_credit(c)
        if step < STEPS - 2:
            for side in (LO, HI):
                lon_bulk(1 - slot, side, c).start()
            return

        def send(r):
            f = c * parts + r

            @pl.when(jnp.logical_not(start))
            def _():
                lon_fine(LO, f).start()

            @pl.when(f >= fine - lead)
            def _():
                lon_fine(HI, f - (fine - lead)).start()

        loop(parts, send)

    def march_last(c, r):
        slot = (STEPS - 1) % 2
        f = c * parts + r
        lon_both(f * some, some, lon_recv.at[f]).wait_recv()
        loop(some, lambda q: advance(slot, f * some + q, put_end))

        @pl.when(f < fine - lead)
        def _():
            lon_fine(HI, f + lead).start()

        @pl.when(f < fine - 1)
        def _():
            pass_on(total_copy(f), lambda: loop(some, lambda q: add_up(f * some + q, slice(None))))

        @pl.when(f == fine - 1)
        def _():
            for j in range(J - some, J):
                for p in range(PIECES):
                    size = K // PIECES
                    pass_on(piece_copy(j, p), lambda: add_up(j, slice(p * size, (p + 1) * size)))

        @pl.when(start)
        def _():
            lon_fine(LO, f).start()

    def march_end(c):
        end_receives((STEPS - 1) % 2, c)
        loop(parts, lambda r: march_last(c, r))

    load_crowd().wait()
    for step in range(STEPS - 1):
        loop(chunks, lambda c: march(step, c))
        lon_all(step % 2).wait_send()
        lev_all(step % 2).wait_send()
    loop(chunks, march_end)
    slot = (STEPS - 1) % 2
    lon_all(slot).wait_send()
    lev_all(slot).wait_send()
    for side in (LO, HI):
        lat_copy(slot, side).wait_send()

    @pl.when(jnp.logical_not(end))
    def _():
        total_all().wait_send()


def store(size, density_end, carry, running, end, sums, sems):
    J, I, K, L = density_end.shape
    rows, chunks = cut(J, STORES)
    share = 1.0 / size

    def end_copy(own):
        return pltpu.make_async_copy(density_end.at[own], end.at[own], sems.at[0])

    def running_copy(own):
        return pltpu.make_async_copy(sums.at[own], running.at[own], sems.at[1])

    loop(chunks, lambda c: end_copy(pl.ds(c * rows, rows)).start())

    def add_up(j):
        so_far = carry[j]
        for i in range(I):
            so_far = so_far + density_end[j, i] * share
            sums[j, i] = so_far

    def some(c):
        loop(rows, lambda r: add_up(c * rows + r))
        running_copy(pl.ds(c * rows, rows)).start()

    loop(chunks, some)
    end_copy(pl.ds(0, J)).wait()
    running_copy(pl.ds(0, J)).wait()


def body(sizes, density, crowding):
    J, I, K, L = density.shape
    rows, chunks = cut(J, BULK)
    some, parts = cut(rows, max(1, FINE // chunks))
    fine = chunks * parts
    batches, spans = cut(chunks, LOADS)[1], cut(chunks, EDGES)[1]
    dma = pltpu.SemaphoreType.DMA
    whole = jax.ShapeDtypeStruct(density.shape, jnp.float32)
    vmem = pl.BlockSpec(memory_space=pltpu.VMEM)
    hbm = pl.BlockSpec(memory_space=pl.ANY)
    carry, density_end = pl.pallas_call(
        functools.partial(kernel, sizes),
        out_shape=(pltpu.VMEM((J, K, L), jnp.float32), pltpu.VMEM(density.shape, jnp.float32)),
        in_specs=[hbm] * 2,
        out_specs=(vmem,) * 2,
        scratch_shapes=[
            pltpu.VMEM((2, J + 2, I, K, L), jnp.float32),
            pltpu.VMEM((J, I, K, L), jnp.float32),
            pltpu.VMEM((2, J, K, L), jnp.float32),
            pltpu.VMEM((J, K, L), jnp.float32),
            pltpu.VMEM((J, K, L), jnp.float32),
            pltpu.VMEM((2, 2, J, I, 8, L), jnp.float32),
            dma((batches,)),
            dma,
            dma((2,)),
            dma((fine,)),
            dma((2,)),
            dma((2, spans)),
            dma((2,)),
            dma((2, 2)),
            dma,
            dma((fine,)),
            dma((some, PIECES)),
            pltpu.SemaphoreType.REGULAR((chunks,)),
        ],
        compiler_params=pltpu.CompilerParams(
            collective_id=0, has_side_effects=True, vmem_limit_bytes=40 * 2**20
        ),
    )(density, crowding)
    return pl.pallas_call(
        functools.partial(store, I * sizes[1]),
        out_shape=(whole, whole),
        in_specs=[vmem] * 2,
        out_specs=(hbm,) * 2,
        scratch_shapes=[pltpu.VMEM(density.shape, jnp.float32), dma((2,))],
        compiler_params=pltpu.CompilerParams(vmem_limit_bytes=10 * 2**20),
    )(density_end, carry)


def solution(mesh):
    sizes = tuple(mesh.shape[name] for name in ("lat", "lon", "lev"))
    return jax.shard_map(
        functools.partial(body, sizes),
        mesh=mesh,
        in_specs=(P("lat", "lon", "lev", None), P("lat", "lon", "lev", None)),
        out_specs=(P("lat", "lon", "lev", None), P("lat", "lon", "lev", None)),
        check_vma=False,
    )
```
